32 devices in a mesh: rep: 2 (over y), span: 2 (over core), seq: 4 (over z), tp: 2 (over x).
Axes of the slice: x: 2, y: 2, z: 4, core: 2. Of those that a mesh axis runs over, the one named last changes fastest.
Arguments:
- queries: bfloat16 [8, 512, 24, 128], P(('rep', 'span'), 'seq', 'tp'), parts along dimension 0, may hold values from -110 to 110
- key_states: bfloat16 [8, 512, 4, 128], P(('rep', 'span'), 'seq', 'tp'), parts along dimension 0, may hold values from -11 to 11
- value_states: bfloat16 [8, 512, 4, 128], P(('rep', 'span'), 'seq', 'tp'), parts along dimension 0, may hold values from -6 to 6
- out_weight: bfloat16 [3072, 6144], P('tp', 'seq'), may hold values from -0.109375 to 0.109375
- noise_table: float32 [64, 6144], P(None, 'tp'), may hold values from 0.5 to 2
- plan: int32 [8], P('rep'), parts along dimension 0, may hold values from 0 to 63
Outputs:
- branch_out: bfloat16 [8, 512, 6144], P(('rep', 'span'), 'seq', 'tp'), parts along dimension 0
The draws below stay inside these ranges and needn't reach their ends.
There are 2 independent parts, one for each index of `rep`. The reference program is written for one: setup_inputs(seed, part) draws one part's arguments, and reference() takes and returns one part's arrays. A program takes and returns all parts, laid end to end along the dimension named above; an argument that names none is the same for every part. Nothing has to cross between parts.
All inputs are finite; a program needn't handle non-finite values.
Results may differ from the reference program's by a relative error of at most 0.014.
Values may be sent and summed in bfloat16 or wider, within the bound.
A program may use at most 128 MiB of HBM per device.

```python
import jax
import jax.numpy as jnp
from jax import lax

D = 6144
QH = 24
KVH = 4
HD = 128
STEPS = 64
SPANS = 4
CTOK = 512


def draw_together(key):
    base = jax.random.fold_in(key, 11)
    first, second = jax.random.split(base, 2)
    query_all = 1.6 * jax.random.truncated_normal(first, -6.0, 6.0, (SPANS, CTOK, QH, HD), jnp.float32)
    key_all = 1.6 * jax.random.truncated_normal(second, -6.0, 6.0, (SPANS, CTOK, KVH, HD), jnp.float32)
    return (query_all, key_all)


def draw_queries(key, part):
    return draw_together(key)[0].astype(jnp.bfloat16)


def draw_key_states(key, part):
    return draw_together(key)[1].astype(jnp.bfloat16)


def place_ends(drawn, own_key, least, top_value):
    place = [jax.random.randint(jax.random.fold_in(own_key, axis), (), 0, length) for axis, length in enumerate(drawn.shape)]
    widest = drawn.shape.index(max(drawn.shape))
    next_to = place[:widest] + [(place[widest] + 1) % drawn.shape[widest]] + place[widest + 1:]
    return drawn.at[tuple(place)].set(least).at[tuple(next_to)].set(top_value)


def block_scale(rng, dims, cuts, low, top_value):
    factor_of, own = 1.0, jax.random.fold_in(rng, 6)
    for axis_at, blocks in cuts:
        steps = jnp.exp(jax.random.uniform(jax.random.fold_in(own, axis_at), (blocks,), jnp.float32, low / len(cuts), top_value / len(cuts)))
        factor_of = factor_of * jnp.repeat(steps, dims[axis_at] // blocks).reshape([-1 if axis == axis_at else 1 for axis in range(len(dims))])
    return factor_of


def bell_draw(stream_key, extent, width, reach, cuts=(), kind=jnp.bfloat16):
    values = width * jax.random.normal(stream_key, extent, jnp.float32)
    if cuts:
        values = values * block_scale(stream_key, extent, cuts, -0.22, 0.18)
    return jnp.clip(values, -reach, reach).astype(kind)


def setup_inputs(seed: int = 0, part: int = 0) -> dict:
    arg_keys = jax.random.split(jax.random.key(seed), 7)
    part_splits = jax.random.split(jax.random.fold_in(arg_keys[6], part), 7)
    return {
        "queries": draw_queries(jax.random.fold_in(jax.random.fold_in(arg_keys[6], part), 71), part),
        "key_states": draw_key_states(jax.random.fold_in(jax.random.fold_in(arg_keys[6], part), 71), part),
        "value_states": bell_draw(part_splits[2], (SPANS, CTOK, KVH, HD), 1.0, 6.0, ((0, 2), (1, 4), (2, 2))),
        "out_weight": bell_draw(arg_keys[3], (QH * HD, D), (QH * HD) ** -0.5, 0.109375, ((0, 2), (1, 4))),
        "noise_table": jnp.clip(0.5 + 1.5 * jax.random.uniform(arg_keys[4], (STEPS, D), jnp.float32) ** block_scale(arg_keys[4], (STEPS, D), ((1, 2),), -0.2, 0.2), 0.5, 2.0),
        "plan": place_ends(jax.random.randint(part_splits[5], (SPANS,), 0, STEPS), jax.random.fold_in(part_splits[5], 1), 0, STEPS - 1).astype(jnp.int32),
    }


def reference(queries, key_states, value_states, out_weight, noise_table, plan):
    per_kv = QH // KVH
    factor = HD ** -0.5
    pieces = []
    for span in range(SPANS):
        key_all = key_states[:span + 1].reshape((span + 1) * CTOK, KVH, HD)
        value_all = value_states[:span + 1].reshape((span + 1) * CTOK, KVH, HD)

        def head_attend(head, span=span, key_all=key_all, value_all=value_all):
            owner = (head // per_kv).astype(jnp.int32)
            query_rows = lax.dynamic_index_in_dim(queries[span], head, 1, keepdims=False)
            key_rows = lax.dynamic_index_in_dim(key_all, owner, 1, keepdims=False)
            value_rows = lax.dynamic_index_in_dim(value_all, owner, 1, keepdims=False)
            scores = jnp.dot(query_rows, key_rows.T, preferred_element_type=jnp.float32) * factor
            highest = jnp.max(scores, axis=1, keepdims=True)
            weights = jnp.exp(scores - highest)
            totals = jnp.sum(weights, axis=1, keepdims=True)
            mixed = jnp.dot(weights.astype(jnp.bfloat16), value_rows, preferred_element_type=jnp.float32)
            return mixed / totals

        heads_out = lax.map(head_attend, jnp.arange(QH, dtype=jnp.int32))
        pieces.append(jnp.transpose(heads_out, (1, 0, 2)).reshape(CTOK, QH * HD).astype(jnp.bfloat16))
    attn = jnp.stack(pieces)
    projected = jnp.dot(attn.reshape(SPANS * CTOK, QH * HD), out_weight, preferred_element_type=jnp.float32).reshape(SPANS, CTOK, D)
    picks = (plan[:, None] == jnp.arange(STEPS, dtype=jnp.int32)[None, :]).astype(jnp.float32)
    gates = jnp.dot(picks, noise_table, precision=lax.Precision.HIGHEST)
    return (projected * gates[:, None, :]).astype(jnp.bfloat16)
```

```python
import functools
import math

import jax
import jax.numpy as jnp
from jax import lax
from jax.experimental import pallas as pl
from jax.experimental.pallas import tpu as pltpu
from jax.sharding import PartitionSpec as P

MESH = pl.DeviceIdType.MESH


def fused_kernel(
    parts, plan_ref, q_ref, kv_ref, noise_ref, w_ref, out_ref,
    kvbuf, wbuf, abuf, pbuf, xsend, xbuf,
    kv_send, kv_recv, kvc, loc, wz_send, wc_send, wy_send,
    wz_recv, wc_recv, wy_recv, x_send, x_recv,
):
    y, c = lax.axis_index("rep"), lax.axis_index("span")
    z, t = lax.axis_index("seq"), lax.axis_index("tp")
    n = lax.axis_size("seq")
    cores, tps = lax.axis_size("span"), lax.axis_size("tp")
    spans, heads, tok, hd = q_ref.shape
    kvh = kv_ref.shape[1]
    per_kv = heads // kvh
    depth, cols = w_ref.shape
    quarter = depth // (cores * lax.axis_size("rep"))
    sub = cols // parts
    owned = n // tps
    first = c * spans
    steps = (n - 1) * parts
    scale = hd ** (-0.5) * math.log2(math.e)

    def rows(yy, cc):
        return pl.ds(pl.multiple_of((yy * cores + cc) * quarter, quarter), quarter)

    def remote(src, dst, send, recv, where):
        return pltpu.make_async_remote_copy(
            src_ref=src, dst_ref=dst, send_sem=send, recv_sem=recv,
            device_id=where, device_id_type=MESH,
        )

    def z_copy(s, j, way, own):
        dst = wbuf.at[s, j, rows(y, c)]
        src = w_ref.at[rows(y, c), pl.ds(pl.multiple_of(j * sub, sub), sub)] if own else dst
        to = z - 1 if way == 0 else z + 1
        return remote(src, dst, wz_send.at[way, s, j], wz_recv.at[s, j], {"seq": to})

    def core_copy(s, j, kind):
        part = wbuf.at[s, j, rows(y if kind == 0 else 1 - y, c)]
        return remote(part, part, wc_send.at[kind, s, j], wc_recv.at[kind, s, j], {"span": 1 - c})

    def y_copy(s, j):
        part = wbuf.at[s, j, rows(y, c)]
        return remote(part, part, wy_send.at[s, j], wy_recv.at[s, j], {"rep": 1 - y})

    def x_copy(s, j):
        at = lax.rem(s, owned)
        return remote(xsend.at[at, j], xbuf.at[at, j], x_send.at[at, j], x_recv.at[at, j], {"tp": 1 - t})

    def kv_copy(to, at):
        return remote(
            kv_ref, kvbuf.at[pl.ds(first, spans), :, :, z], kv_send.at[to], kv_recv.at[at], {"seq": to}
        )

    def kv_core():
        part = kvbuf.at[pl.ds(0, spans)]
        return remote(part, part, kvc.at[0], kvc.at[1], {"span": 1 - c})

    def local_w(j):
        return pltpu.make_async_copy(
            w_ref.at[:, pl.ds(pl.multiple_of(j * sub, sub), sub)], wbuf.at[z, j], loc.at[j]
        )

    def local_kv():
        return pltpu.make_async_copy(
            kv_ref, kvbuf.at[pl.ds(first, spans), :, :, z], loc.at[parts]
        )

    barrier = pltpu.get_barrier_semaphore()
    for peer in range(n):
        @pl.when(z != peer)
        def _(peer=peer):
            pl.semaphore_signal(barrier, inc=1, device_id={"seq": peer}, device_id_type=MESH)
    pl.semaphore_signal(barrier, inc=1, device_id={"rep": 1 - y}, device_id_type=MESH)
    pl.semaphore_signal(barrier, inc=1, device_id={"span": 1 - c}, device_id_type=MESH)
    pl.semaphore_signal(barrier, inc=1, device_id={"tp": 1 - t}, device_id_type=MESH)
    pl.semaphore_wait(barrier, n - 1 + 3)

    local_kv().start()
    for peer in range(n):
        @pl.when(z != peer)
        def _(peer=peer):
            kv_copy(peer, z).start()
    for j in range(parts):
        @pl.when(z > 0)
        def _(j=j):
            z_copy(z, j, 0, True).start()

        @pl.when(z < n - 1)
        def _(j=j):
            z_copy(z, j, 1, True).start()
    for j in range(parts):
        local_w(j).start()

    local_kv().wait()
    for peer in range(n):
        @pl.when(z != peer)
        def _(peer=peer):
            kv_copy(peer, peer).wait_recv()

    @pl.when(c == 0)
    def _():
        kv_core().start()

    @pl.when(c != 0)
    def _():
        kv_core().wait_recv()

    def each(e, low, do):
        ok = jnp.logical_and(e >= low, e < steps)
        d, j = e // parts + 1, e % parts
        for sign in (-1, 1):
            s = z + sign * d

            @pl.when(jnp.logical_and(ok, jnp.logical_and(s >= 0, s < n)))
            def _(s=s, sign=sign):
                do(s, j, sign)

    def arrive(s, j, sign):
        way = 0 if sign > 0 else 1
        z_copy(s, j, way, False).wait_recv()

        @pl.when((z > 0) if way == 0 else (z < n - 1))
        def _():
            z_copy(s, j, way, False).start()

        y_copy(s, j).start()
        core_copy(s, j, 0).start()

    def pass_on(s, j, sign):
        y_copy(s, j).wait_recv()
        core_copy(s, j, 1).start()

    def project(s, j):
        part = jnp.dot(abuf[...], wbuf[s, j], preferred_element_type=jnp.float32)
        at = lax.rem(s, owned)

        @pl.when(s // owned == t)
        def _():
            pbuf[at, j] = part

        @pl.when(s // owned != t)
        def _():
            xsend[at, j] = part.astype(jnp.bfloat16)
            x_copy(s, j).start()

    def gather_project(s, j, sign):
        core_copy(s, j, 0).wait_recv()
        core_copy(s, j, 1).wait_recv()
        project(s, j)

    def finish(s, j, sign):
        @pl.when(s // owned == t)
        def _():
            x_copy(s, j).wait_recv()
            at = lax.rem(s, owned)
            where = pl.ds(pl.multiple_of(at * cols + j * sub, 128), sub)
            for i in range(spans):
                level = plan_ref[first + i]
                gate = noise_ref[pl.ds(level, 1), where]
                mine = pl.ds(i * tok, tok)
                total = pbuf[at, j, mine, :] + xbuf[at, j, mine, :].astype(jnp.float32)
                out_ref[mine, where] = (total * gate).astype(out_ref.dtype)

    units = spans * kvh
    lead = per_kv * tok

    def attend(u, carry):
        i, g = u // kvh, u % kvh
        query = q_ref[i, pl.ds(g * per_kv, per_kv)].reshape(lead, hd)

        def fold(k, state):
            top, total, mixed = state
            keys = kvbuf[k, g, 0].reshape(n * tok, hd)
            values = kvbuf[k, g, 1].reshape(n * tok, hd)
            scores = lax.dot_general(
                query, keys, (((1,), (1,)), ((), ())), preferred_element_type=jnp.float32
            )
            high = jnp.maximum(top, jnp.max(scores, axis=1, keepdims=True))
            shrink = jnp.exp2((top - high) * scale)
            weights = jnp.exp2((scores - high) * scale)
            total = total * shrink + jnp.sum(weights, axis=1, keepdims=True)
            mixed = mixed * shrink + jnp.dot(
                weights.astype(jnp.bfloat16), values, preferred_element_type=jnp.float32
            )
            return high, total, mixed

        start = (
            jnp.full((lead, 1), -1e30, jnp.float32),
            jnp.zeros((lead, 1), jnp.float32),
            jnp.zeros((lead, hd), jnp.float32),
        )
        _, total, mixed = lax.fori_loop(0, first + i + 1, fold, start)
        result = (mixed / total).astype(jnp.bfloat16).reshape(per_kv, tok, hd)
        for h in range(per_kv):
            abuf[
                pl.ds(pl.multiple_of(i * tok, tok), tok),
                pl.ds(pl.multiple_of((g * per_kv + h) * hd, hd), hd),
            ] = result[h]
        each(u, 0, arrive)
        each(u - 1, 0, pass_on)
        return carry

    lax.fori_loop(0, units, attend, 0)

    def own(j, carry):
        local_w(j).wait()
        project(z, j)
        return carry

    lax.fori_loop(0, parts, own, 0)

    def run(e, carry):
        each(e, units, arrive)
        each(e - 1, units - 1, pass_on)
        each(e - 2, 0, gather_project)
        each(e - 3, 0, finish)
        return carry

    lax.fori_loop(2, units, lambda e, carry: (each(e - 2, 0, gather_project), carry)[1], 0)
    lax.fori_loop(0, parts, lambda j, carry: (finish(z, j, 0), carry)[1], 0)
    lax.fori_loop(3, units, lambda e, carry: (each(e - 3, 0, finish), carry)[1], 0)
    lax.fori_loop(units, max(steps, units) + 3, run, 0)

    for peer in range(n):
        @pl.when(z != peer)
        def _(peer=peer):
            kv_copy(peer, z).wait_send()

    @pl.when(c == 0)
    def _():
        kv_core().wait_send()

    def drain(f, carry):
        s, j = f // parts, f % parts

        @pl.when(jnp.logical_and(z > 0, s >= z))
        def _():
            z_copy(s, j, 0, False).wait_send()

        @pl.when(jnp.logical_and(z < n - 1, s <= z))
        def _():
            z_copy(s, j, 1, False).wait_send()

        @pl.when(s != z)
        def _():
            core_copy(s, j, 0).wait_send()
            core_copy(s, j, 1).wait_send()
            y_copy(s, j).wait_send()

        @pl.when(s // owned != t)
        def _():
            x_copy(s, j).wait_send()

        return carry

    lax.fori_loop(0, n * parts, drain, 0)


def fused(parts, queries, key_states, value_states, out_weight, noise_table, plan):
    spans, tok, heads, hd = queries.shape
    kvh = key_states.shape[2]
    depth, cols = out_weight.shape
    n, tps, cores = lax.axis_size("seq"), lax.axis_size("tp"), lax.axis_size("span")
    sub, owned, wide = cols // parts, n // tps, noise_table.shape[1]
    q = jnp.transpose(queries, (0, 2, 1, 3))
    kv = jnp.stack([key_states, value_states], axis=0).transpose(1, 3, 0, 2, 4)
    vmem = pl.BlockSpec(memory_space=pltpu.VMEM)
    dma = pltpu.SemaphoreType.DMA
    out = pl.pallas_call(
        functools.partial(fused_kernel, parts),
        out_shape=jax.ShapeDtypeStruct((spans * tok, wide), jnp.bfloat16),
        in_specs=[
            pl.BlockSpec(memory_space=pltpu.SMEM), vmem, vmem, vmem,
            pl.BlockSpec(memory_space=pl.ANY),
        ],
        out_specs=vmem,
        scratch_shapes=[
            pltpu.VMEM((spans * cores, kvh, 2, n, tok, hd), jnp.bfloat16),
            pltpu.VMEM((n, parts, depth, sub), jnp.bfloat16),
            pltpu.VMEM((spans * tok, depth), jnp.bfloat16),
            pltpu.VMEM((owned, parts, spans * tok, sub), jnp.float32),
            pltpu.VMEM((owned, parts, spans * tok, sub), jnp.bfloat16),
            pltpu.VMEM((owned, parts, spans * tok, sub), jnp.bfloat16),
            dma((n,)), dma((n,)), dma((2,)), dma((parts + 1,)),
            dma((2, n, parts)), dma((2, n, parts)), dma((n, parts)),
            dma((n, parts)), dma((2, n, parts)), dma((n, parts)),
            dma((owned, parts)), dma((owned, parts)),
        ],
        compiler_params=pltpu.CompilerParams(
            collective_id=0, has_side_effects=True, vmem_limit_bytes=60 * 1024 * 1024
        ),
        name="relay_attention",
    )(plan, q, kv, noise_table, out_weight)
    return out.reshape(spans, tok, wide)


def fold_block(carried, query_rows, key_rows, value_rows, factor):
    maxima, totals, weighted = carried
    scores = (
        jnp.einsum("tkgd,skd->tkgs", query_rows, key_rows, preferred_element_type=jnp.float32)
        * factor
    )
    highest = jnp.maximum(maxima, jnp.max(scores, axis=-1))
    shrink = jnp.exp(maxima - highest)
    weights = jnp.exp(scores - highest[..., None])
    totals = totals * shrink + jnp.sum(weights, axis=-1)
    weighted = weighted * shrink[..., None] + jnp.einsum(
        "tkgs,skd->tkgd",
        weights.astype(jnp.bfloat16),
        value_rows,
        preferred_element_type=jnp.float32,
    )
    return (maxima * 0.0 + highest, totals, weighted)


def per_device(queries, key_states, value_states, out_weight, noise_table, plan):
    ch_dev, tok_dev, heads_local, head_size = queries.shape
    kv_local = key_states.shape[2]
    per_kv = heads_local // kv_local
    span_count = ch_dev * lax.axis_size("span")
    first_span = lax.axis_index("span") * ch_dev
    factor = head_size ** (-0.5)
    grouped = queries.reshape(ch_dev, tok_dev, kv_local, per_kv, head_size)
    start_max = jnp.full((ch_dev, tok_dev, kv_local, per_kv), -1e30, jnp.float32)
    start_tot = jnp.zeros((ch_dev, tok_dev, kv_local, per_kv), jnp.float32)
    start_acc = jnp.zeros((ch_dev, tok_dev, kv_local, per_kv, head_size), jnp.float32)
    span_rows = (
        lax.all_gather(key_states, "seq", axis=1, tiled=True),
        lax.all_gather(value_states, "seq", axis=1, tiled=True),
    )
    key_piece = lax.all_gather(span_rows[0], "span", axis=0, tiled=True)
    value_piece = lax.all_gather(span_rows[1], "span", axis=0, tiled=True)
    new_max = []
    new_tot = []
    new_acc = []
    for q_span in range(ch_dev):
        inner_state = (start_max[q_span], start_tot[q_span], start_acc[q_span])
        for k_span in range(span_count):

            def update(inner, q_span=q_span, k_span=k_span):
                return fold_block(
                    inner, grouped[q_span], key_piece[k_span], value_piece[k_span], factor
                )

            inner_state = lax.cond(
                k_span <= first_span + q_span, update, lambda inner: inner, inner_state
            )
        new_max.append(inner_state[0])
        new_tot.append(inner_state[1])
        new_acc.append(inner_state[2])
    attn = (
        (jnp.stack(new_acc) / jnp.stack(new_tot)[..., None])
        .reshape(ch_dev, tok_dev, heads_local * head_size)
        .astype(jnp.bfloat16)
    )
    columns = jnp.einsum(
        "ctf,fo->cto",
        lax.all_gather(attn, "seq", axis=1, tiled=True),
        out_weight,
        preferred_element_type=jnp.float32,
    )
    partial_out = lax.all_to_all(
        columns.astype(jnp.bfloat16), "seq", split_axis=1, concat_axis=2, tiled=True
    ).astype(columns.dtype)
    summed = lax.psum_scatter(
        partial_out.astype(jnp.bfloat16), "tp", scatter_dimension=2, tiled=True
    ).astype(jnp.float32)
    levels = lax.dynamic_slice_in_dim(plan, first_span, ch_dev)
    picks = (levels[:, None] == jnp.arange(noise_table.shape[0], dtype=jnp.int32)[None, :]).astype(
        jnp.float32
    )
    gates = jnp.dot(picks, noise_table, precision=lax.Precision.HIGHEST)
    return (summed * gates[:, None, :]).astype(jnp.bfloat16)


def choose_parts(cols):
    for parts in (4, 3, 2, 1):
        if cols % (parts * 128) == 0:
            return parts
    return 0


def dispatch(queries, key_states, value_states, out_weight, noise_table, plan):
    depth, cols = out_weight.shape
    copies = lax.axis_size("rep") * lax.axis_size("span")
    parts = choose_parts(cols)
    pairs = all(lax.axis_size(name) == 2 for name in ("rep", "span", "tp"))
    args = (queries, key_states, value_states, out_weight, noise_table, plan)
    if pairs and parts and depth % (copies * 16) == 0 and lax.axis_size("seq") % 2 == 0:
        return fused(parts, *args)
    return per_device(*args)


def solution(mesh):
    placed = (
        P(("rep", "span"), "seq", "tp", None),
        P(("rep", "span"), "seq", "tp", None),
        P(("rep", "span"), "seq", "tp", None),
        P("tp", "seq"),
        P(None, "tp"),
        P("rep"),
    )
    return jax.shard_map(
        dispatch,
        mesh=mesh,
        in_specs=placed,
        out_specs=P(("rep", "span"), "seq", "tp"),
        check_vma=False,
    )
```

```python
import functools
import math

import jax
import jax.numpy as jnp
from jax import lax
from jax.experimental import pallas as pl
from jax.experimental.pallas import tpu as pltpu
from jax.sharding import PartitionSpec as P

MESH = pl.DeviceIdType.MESH


def fused_kernel(
    parts, plan_ref, q_ref, kv_ref, noise_ref, w_ref, out_ref,
    kvbuf, wbuf, abuf, pbuf, xsend, xbuf,
    kv_send, kv_recv, kvc, loc, wz_send, wc_send, wy_send,
    wz_recv, wc_recv, wy_recv, x_send, x_recv,
):
    y, c = lax.axis_index("rep"), lax.axis_index("span")
    z, t = lax.axis_index("seq"), lax.axis_index("tp")
    n = lax.axis_size("seq")
    cores, tps = lax.axis_size("span"), lax.axis_size("tp")
    spans, heads, tok, hd = q_ref.shape
    kvh = kv_ref.shape[1]
    per_kv = heads // kvh
    depth, cols = w_ref.shape
    quarter = depth // (cores * lax.axis_size("rep"))
    sub = cols // parts
    owned = n // tps
    first = c * spans
    steps = (n - 1) * parts
    scale = hd ** (-0.5) * math.log2(math.e)

    def rows(yy, cc):
        return pl.ds(pl.multiple_of((yy * cores + cc) * quarter, quarter), quarter)

    def remote(src, dst, send, recv, where):
        return pltpu.make_async_remote_copy(
            src_ref=src, dst_ref=dst, send_sem=send, recv_sem=recv,
            device_id=where, device_id_type=MESH,
        )

    def z_copy(s, j, way, own):
        dst = wbuf.at[s, j, rows(y, c)]
        src = w_ref.at[rows(y, c), pl.ds(pl.multiple_of(j * sub, sub), sub)] if own else dst
        to = z - 1 if way == 0 else z + 1
        return remote(src, dst, wz_send.at[way, s, j], wz_recv.at[s, j], {"seq": to})

    def core_copy(s, j, kind):
        part = wbuf.at[s, j, rows(y if kind == 0 else 1 - y, c)]
        return remote(part, part, wc_send.at[kind, s, j], wc_recv.at[kind, s, j], {"span": 1 - c})

    def y_copy(s, j):
        part = wbuf.at[s, j, rows(y, c)]
        return remote(part, part, wy_send.at[s, j], wy_recv.at[s, j], {"rep": 1 - y})

    def x_copy(s, j):
        at = lax.rem(s, owned)
        return remote(xsend.at[at, j], xbuf.at[at, j], x_send.at[at, j], x_recv.at[at, j], {"tp": 1 - t})

    def kv_copy(to, at):
        return remote(
            kv_ref, kvbuf.at[pl.ds(first, spans), :, :, z], kv_send.at[to], kv_recv.at[at], {"seq": to}
        )

    def kv_core():
        part = kvbuf.at[pl.ds(0, spans)]
        return remote(part, part, kvc.at[0], kvc.at[1], {"span": 1 - c})

    def local_w(j):
        return pltpu.make_async_copy(
            w_ref.at[:, pl.ds(pl.multiple_of(j * sub, sub), sub)], wbuf.at[z, j], loc.at[j]
        )

    def local_kv():
        return pltpu.make_async_copy(
            kv_ref, kvbuf.at[pl.ds(first, spans), :, :, z], loc.at[parts]
        )

    barrier = pltpu.get_barrier_semaphore()
    for peer in range(n):
        @pl.when(z != peer)
        def _(peer=peer):
            pl.semaphore_signal(barrier, inc=1, device_id={"seq": peer}, device_id_type=MESH)
    pl.semaphore_signal(barrier, inc=1, device_id={"rep": 1 - y}, device_id_type=MESH)
    pl.semaphore_signal(barrier, inc=1, device_id={"span": 1 - c}, device_id_type=MESH)
    pl.semaphore_signal(barrier, inc=1, device_id={"tp": 1 - t}, device_id_type=MESH)
    pl.semaphore_wait(barrier, n - 1 + 3)

    local_kv().start()
    for peer in range(n):
        @pl.when(z != peer)
        def _(peer=peer):
            kv_copy(peer, z).start()
    for j in range(parts):
        @pl.when(z > 0)
        def _(j=j):
            z_copy(z, j, 0, True).start()

        @pl.when(z < n - 1)
        def _(j=j):
            z_copy(z, j, 1, True).start()
    for j in range(parts):
        local_w(j).start()

    local_kv().wait()
    for peer in range(n):
        @pl.when(z != peer)
        def _(peer=peer):
            kv_copy(peer, peer).wait_recv()

    @pl.when(c == 0)
    def _():
        kv_core().start()

    @pl.when(c != 0)
    def _():
        kv_core().wait_recv()

    def each(e, low, do):
        ok = jnp.logical_and(e >= low, e < steps)
        d, j = e // parts + 1, e % parts
        for sign in (-1, 1):
            s = z + sign * d

            @pl.when(jnp.logical_and(ok, jnp.logical_and(s >= 0, s < n)))
            def _(s=s, sign=sign):
                do(s, j, sign)

    def arrive(s, j, sign):
        way = 0 if sign > 0 else 1
        z_copy(s, j, way, False).wait_recv()

        @pl.when((z > 0) if way == 0 else (z < n - 1))
        def _():
            z_copy(s, j, way, False).start()

        y_copy(s, j).start()
        core_copy(s, j, 0).start()

    def pass_on(s, j, sign):
        y_copy(s, j).wait_recv()
        core_copy(s, j, 1).start()

    def project(s, j):
        part = jnp.dot(abuf[...], wbuf[s, j], preferred_element_type=jnp.float32)
        at = lax.rem(s, owned)

        @pl.when(s // owned == t)
        def _():
            pbuf[at, j] = part

        @pl.when(s // owned != t)
        def _():
            xsend[at, j] = part.astype(jnp.bfloat16)
            x_copy(s, j).start()

    def gather_project(s, j, sign):
        core_copy(s, j, 0).wait_recv()
        core_copy(s, j, 1).wait_recv()
        project(s, j)

    def finish(s, j, sign):
        @pl.when(s // owned == t)
        def _():
            x_copy(s, j).wait_recv()
            at = lax.rem(s, owned)
            where = pl.ds(pl.multiple_of(at * cols + j * sub, 128), sub)
            for i in range(spans):
                level = plan_ref[first + i]
                gate = noise_ref[pl.ds(level, 1), where]
                mine = pl.ds(i * tok, tok)
                total = pbuf[at, j, mine, :] + xbuf[at, j, mine, :].astype(jnp.float32)
                out_ref[mine, where] = (total * gate).astype(out_ref.dtype)

    units = spans * kvh
    lag = units - 1
    lead = per_kv * tok

    def attend(u, carry):
        i, g = u // kvh, u % kvh
        query = q_ref[i, pl.ds(g * per_kv, per_kv)].reshape(lead, hd)

        def fold(k, state):
            top, total, mixed = state
            keys = kvbuf[k, g, 0].reshape(n * tok, hd)
            values = kvbuf[k, g, 1].reshape(n * tok, hd)
            scores = lax.dot_general(
                query, keys, (((1,), (1,)), ((), ())), preferred_element_type=jnp.float32
            )
            high = jnp.maximum(top, jnp.max(scores, axis=1, keepdims=True))
            shrink = jnp.exp2((top - high) * scale)
            weights = jnp.exp2((scores - high) * scale)
            total = total * shrink + jnp.sum(weights, axis=1, keepdims=True)
            mixed = mixed * shrink + jnp.dot(
                weights.astype(jnp.bfloat16), values, preferred_element_type=jnp.float32
            )
            return high, total, mixed

        start = (
            jnp.full((lead, 1), -1e30, jnp.float32),
            jnp.zeros((lead, 1), jnp.float32),
            jnp.zeros((lead, hd), jnp.float32),
        )
        _, total, mixed = lax.fori_loop(0, first + i + 1, fold, start)
        result = (mixed / total).astype(jnp.bfloat16).reshape(per_kv, tok, hd)
        for h in range(per_kv):
            abuf[
                pl.ds(pl.multiple_of(i * tok, tok), tok),
                pl.ds(pl.multiple_of((g * per_kv + h) * hd, hd), hd),
            ] = result[h]
        each(u, 0, arrive)
        each(u - lag, 0, pass_on)
        return carry

    lax.fori_loop(0, units, attend, 0)

    def own(j, carry):
        local_w(j).wait()
        project(z, j)
        return carry

    lax.fori_loop(0, parts, own, 0)

    def run(e, carry):
        each(e, units, arrive)
        each(e - lag, units - lag, pass_on)
        each(e - lag - 1, 0, gather_project)
        each(e - lag - 3, 0, finish)
        return carry

    lax.fori_loop(0, parts, lambda j, carry: (finish(z, j, 0), carry)[1], 0)
    lax.fori_loop(units, max(steps, units) + lag + 3, run, 0)

    for peer in range(n):
        @pl.when(z != peer)
        def _(peer=peer):
            kv_copy(peer, z).wait_send()

    @pl.when(c == 0)
    def _():
        kv_core().wait_send()

    def drain(f, carry):
        s, j = f // parts, f % parts

        @pl.when(jnp.logical_and(z > 0, s >= z))
        def _():
            z_copy(s, j, 0, False).wait_send()

        @pl.when(jnp.logical_and(z < n - 1, s <= z))
        def _():
            z_copy(s, j, 1, False).wait_send()

        @pl.when(s != z)
        def _():
            core_copy(s, j, 0).wait_send()
            core_copy(s, j, 1).wait_send()
            y_copy(s, j).wait_send()

        @pl.when(s // owned != t)
        def _():
            x_copy(s, j).wait_send()

        return carry

    lax.fori_loop(0, n * parts, drain, 0)


def fused(parts, queries, key_states, value_states, out_weight, noise_table, plan):
    spans, tok, heads, hd = queries.shape
    kvh = key_states.shape[2]
    depth, cols = out_weight.shape
    n, tps, cores = lax.axis_size("seq"), lax.axis_size("tp"), lax.axis_size("span")
    sub, owned, wide = cols // parts, n // tps, noise_table.shape[1]
    q = jnp.transpose(queries, (0, 2, 1, 3))
    kv = jnp.stack([key_states, value_states], axis=0).transpose(1, 3, 0, 2, 4)
    vmem = pl.BlockSpec(memory_space=pltpu.VMEM)
    dma = pltpu.SemaphoreType.DMA
    out = pl.pallas_call(
        functools.partial(fused_kernel, parts),
        out_shape=jax.ShapeDtypeStruct((spans * tok, wide), jnp.bfloat16),
        in_specs=[
            pl.BlockSpec(memory_space=pltpu.SMEM), vmem, vmem, vmem,
            pl.BlockSpec(memory_space=pl.ANY),
        ],
        out_specs=vmem,
        scratch_shapes=[
            pltpu.VMEM((spans * cores, kvh, 2, n, tok, hd), jnp.bfloat16),
            pltpu.VMEM((n, parts, depth, sub), jnp.bfloat16),
            pltpu.VMEM((spans * tok, depth), jnp.bfloat16),
            pltpu.VMEM((owned, parts, spans * tok, sub), jnp.float32),
            pltpu.VMEM((owned, parts, spans * tok, sub), jnp.bfloat16),
            pltpu.VMEM((owned, parts, spans * tok, sub), jnp.bfloat16),
            dma((n,)), dma((n,)), dma((2,)), dma((parts + 1,)),
            dma((2, n, parts)), dma((2, n, parts)), dma((n, parts)),
            dma((n, parts)), dma((2, n, parts)), dma((n, parts)),
            dma((owned, parts)), dma((owned, parts)),
        ],
        compiler_params=pltpu.CompilerParams(
            collective_id=0, has_side_effects=True, vmem_limit_bytes=60 * 1024 * 1024
        ),
        name="relay_attention",
    )(plan, q, kv, noise_table, out_weight)
    return out.reshape(spans, tok, wide)


def fold_block(carried, query_rows, key_rows, value_rows, factor):
    maxima, totals, weighted = carried
    scores = (
        jnp.einsum("tkgd,skd->tkgs", query_rows, key_rows, preferred_element_type=jnp.float32)
        * factor
    )
    highest = jnp.maximum(maxima, jnp.max(scores, axis=-1))
    shrink = jnp.exp(maxima - highest)
    weights = jnp.exp(scores - highest[..., None])
    totals = totals * shrink + jnp.sum(weights, axis=-1)
    weighted = weighted * shrink[..., None] + jnp.einsum(
        "tkgs,skd->tkgd",
        weights.astype(jnp.bfloat16),
        value_rows,
        preferred_element_type=jnp.float32,
    )
    return (maxima * 0.0 + highest, totals, weighted)


def per_device(queries, key_states, value_states, out_weight, noise_table, plan):
    ch_dev, tok_dev, heads_local, head_size = queries.shape
    kv_local = key_states.shape[2]
    per_kv = heads_local // kv_local
    span_count = ch_dev * lax.axis_size("span")
    first_span = lax.axis_index("span") * ch_dev
    factor = head_size ** (-0.5)
    grouped = queries.reshape(ch_dev, tok_dev, kv_local, per_kv, head_size)
    start_max = jnp.full((ch_dev, tok_dev, kv_local, per_kv), -1e30, jnp.float32)
    start_tot = jnp.zeros((ch_dev, tok_dev, kv_local, per_kv), jnp.float32)
    start_acc = jnp.zeros((ch_dev, tok_dev, kv_local, per_kv, head_size), jnp.float32)
    span_rows = (
        lax.all_gather(key_states, "seq", axis=1, tiled=True),
        lax.all_gather(value_states, "seq", axis=1, tiled=True),
    )
    key_piece = lax.all_gather(span_rows[0], "span", axis=0, tiled=True)
    value_piece = lax.all_gather(span_rows[1], "span", axis=0, tiled=True)
    new_max = []
    new_tot = []
    new_acc = []
    for q_span in range(ch_dev):
        inner_state = (start_max[q_span], start_tot[q_span], start_acc[q_span])
        for k_span in range(span_count):

            def update(inner, q_span=q_span, k_span=k_span):
                return fold_block(
                    inner, grouped[q_span], key_piece[k_span], value_piece[k_span], factor
                )

            inner_state = lax.cond(
                k_span <= first_span + q_span, update, lambda inner: inner, inner_state
            )
        new_max.append(inner_state[0])
        new_tot.append(inner_state[1])
        new_acc.append(inner_state[2])
    attn = (
        (jnp.stack(new_acc) / jnp.stack(new_tot)[..., None])
        .reshape(ch_dev, tok_dev, heads_local * head_size)
        .astype(jnp.bfloat16)
    )
    columns = jnp.einsum(
        "ctf,fo->cto",
        lax.all_gather(attn, "seq", axis=1, tiled=True),
        out_weight,
        preferred_element_type=jnp.float32,
    )
    partial_out = lax.all_to_all(
        columns.astype(jnp.bfloat16), "seq", split_axis=1, concat_axis=2, tiled=True
    ).astype(columns.dtype)
    summed = lax.psum_scatter(
        partial_out.astype(jnp.bfloat16), "tp", scatter_dimension=2, tiled=True
    ).astype(jnp.float32)
    levels = lax.dynamic_slice_in_dim(plan, first_span, ch_dev)
    picks = (levels[:, None] == jnp.arange(noise_table.shape[0], dtype=jnp.int32)[None, :]).astype(
        jnp.float32
    )
    gates = jnp.dot(picks, noise_table, precision=lax.Precision.HIGHEST)
    return (summed * gates[:, None, :]).astype(jnp.bfloat16)


def choose_parts(cols):
    for parts in (6, 3, 2, 1):
        if cols % (parts * 128) == 0:
            return parts
    return 0


def dispatch(queries, key_states, value_states, out_weight, noise_table, plan):
    depth, cols = out_weight.shape
    copies = lax.axis_size("rep") * lax.axis_size("span")
    parts = choose_parts(cols)
    pairs = all(lax.axis_size(name) == 2 for name in ("rep", "span", "tp"))
    args = (queries, key_states, value_states, out_weight, noise_table, plan)
    if pairs and parts and depth % (copies * 16) == 0 and lax.axis_size("seq") % 2 == 0:
        return fused(parts, *args)
    return per_device(*args)


def solution(mesh):
    placed = (
        P(("rep", "span"), "seq", "tp", None),
        P(("rep", "span"), "seq", "tp", None),
        P(("rep", "span"), "seq", "tp", None),
        P("tp", "seq"),
        P(None, "tp"),
        P("rep"),
    )
    return jax.shard_map(
        dispatch,
        mesh=mesh,
        in_specs=placed,
        out_specs=P(("rep", "span"), "seq", "tp"),
        check_vma=False,
    )
```
